32 devices in a mesh: node: 8 (over z, x), dev: 4 (over y, core).
Axes of the slice: x: 2, y: 2, z: 4, core: 2. Of those that a mesh axis runs over, the one named last changes fastest.
Arguments:
- kv_pages: bfloat16 [4096, 1, 2, 16, 1024], P(('node', 'dev')), may hold values from -6 to 6
- new_slot: int32 [4096], P(('node', 'dev')), may hold values from 0 to 4095, as said below
- request_rate: float32 [512], P(('node', 'dev')), may hold values from 0.25 to 4
- page_table: int32 [512, 128], P(('node', 'dev')), may hold values from 0 to 4095
Outputs:
- migrated: bfloat16 [4096, 1, 2, 16, 1024], P(('node', 'dev'))
- device_load: float32 [32], replicated
The draws below stay inside these ranges and needn't reach their ends.
Inputs may be any that keep to these rules, and one draw needn't show every extreme that they name: new_slot is a permutation of the slots; slot p lies on device p // 128. Every device sends exactly 31 of its pages to other devices, at most one to any one device, and receives exactly 31 into the slots that its leaving pages free; its other pages keep their slots.
All inputs are finite; a program needn't handle non-finite values.
Results may differ from the reference program's by a relative error of at most 0.001.
Values may be sent and summed in bfloat16 or wider, within the bound.
No kernel may reach another device: no remote copies, remote signals or barrier semaphores. Data moves between devices by JAX's collectives and lax.ppermute only.
A program may use at most 128 MiB of HBM per device.

```python
import math
import jax
import jax.numpy as jnp
import numpy as np

KVH = 8
HD = 128
LAYERS = 1
PAGE_TOK = 16
PPR = 128
PAGE_DEV = 128
REQ_DEV = 16
MOVE_DEV = 31
PAGES = 4096
REQS = 512
N_NODE = 8
N_DEV = 4


def freed_slots(one_key):
    return jax.random.permutation(one_key, PAGE_DEV)[:MOVE_DEV]


def draw_new_slot(key, part):
    device_total = N_NODE * N_DEV
    page_total = PAGE_DEV * device_total
    key_label, key_shift, key_slots = jax.random.split(jax.random.fold_in(key, 17), 3)
    relabel = jax.random.permutation(key_label, device_total).astype(jnp.int32)
    shifts = (jax.random.permutation(key_shift, device_total - 1)[:MOVE_DEV] + 1).astype(jnp.int32)
    slot_keys = jax.random.split(key_slots, device_total)
    freed = jax.vmap(freed_slots)(slot_keys).astype(jnp.int32)
    position = jnp.arange(device_total, dtype=jnp.int32)
    rounds = jnp.broadcast_to(jnp.arange(MOVE_DEV, dtype=jnp.int32)[None, :], (device_total, MOVE_DEV))
    senders = jnp.broadcast_to(relabel[:, None], (device_total, MOVE_DEV))
    takers = relabel[(position[:, None] + shifts[None, :]) % device_total]
    from_index = senders * PAGE_DEV + freed[senders, rounds]
    to_index = takers * PAGE_DEV + freed[takers, rounds]
    base = jnp.arange(page_total, dtype=jnp.int32)
    return base.at[from_index.reshape(-1)].set(to_index.reshape(-1))


def set_ends(array, own_key, least, top_value):
    longest = array.shape.index(max(array.shape))
    spots = []
    for shift in (0, 1):
        where = [jax.random.randint(jax.random.fold_in(own_key, axis), (), 0, length) for axis, length in enumerate(array.shape)]
        where[longest] = (where[longest] + shift) % array.shape[longest]
        spots.append(tuple(where))
    return array.at[spots[0]].set(least).at[spots[1]].set(top_value)


def shard_levels(stream_key, extent, pieces, low, top_value):
    gain, own = 1.0, jax.random.fold_in(stream_key, 6)
    for axis_at, shards_of in pieces:
        heights = jnp.exp(jax.random.uniform(jax.random.fold_in(own, axis_at), (shards_of,), jnp.float32, low / len(pieces), top_value / len(pieces)))
        gain = gain * jnp.repeat(heights, extent[axis_at] // shards_of).reshape([-1 if axis == axis_at else 1 for axis in range(len(extent))])
    return gain


def rank_bounds(number_of, skew):
    loads = [(1 << 20) // math.isqrt(grade ** skew) + 1 for grade in range(1, number_of + 1)]
    deviation = 1 + sum(loads) // (1 << 30)
    return np.cumsum(np.array([max(1, weight // deviation) for weight in loads]))


def skewed_ids(key, dims, number_of, lean):
    grid = rank_bounds(number_of, lean)
    ticket = jax.random.randint(jax.random.fold_in(key, 1), dims, 0, int(grid[number_of - 1]))
    standing = jnp.searchsorted(jnp.asarray(grid, jnp.int32), ticket, side="right")
    return jax.random.permutation(jax.random.fold_in(key, 2), number_of)[standing].astype(jnp.int32)


def normal_values(stream_key, extent, spread, most, pieces=(), kind=jnp.bfloat16):
    values = spread * jax.random.normal(stream_key, extent, jnp.float32)
    if pieces:
        values = values * shard_levels(stream_key, extent, pieces, -0.22, 0.18)
    return jnp.clip(values, -most, most).astype(kind)


def setup_inputs(seed: int = 0) -> dict:
    splits = jax.random.split(jax.random.key(seed), 5)
    return {
        "kv_pages": normal_values(splits[0], (PAGES, LAYERS, 2, PAGE_TOK, KVH * HD), 1.0, 6.0, ((0, 32),)),
        "new_slot": draw_new_slot(jax.random.fold_in(splits[4], 71), 0),
        "request_rate": jnp.clip(jnp.exp(math.log(4.0) - 2.7725887 * jax.random.uniform(splits[2], (REQS,), jnp.float32) ** shard_levels(splits[2], (REQS,), ((0, 32),), -0.2, 0.2)), 0.25, 4.0),
        "page_table": set_ends(skewed_ids(splits[3], (REQS, PPR), PAGES, 2), jax.random.fold_in(splits[3], 3), 0, PAGES - 1).astype(jnp.int32),
    }


def reference(kv_pages, new_slot, request_rate, page_table):
    page_total = kv_pages.shape[0]
    device_total = N_NODE * N_DEV
    source = jnp.zeros((page_total,), jnp.int32).at[new_slot].set(jnp.arange(page_total, dtype=jnp.int32))
    migrated = jnp.take(kv_pages, source, axis=0)
    weights = jnp.broadcast_to(request_rate[:, None], page_table.shape).reshape(-1)
    page_warmth = jnp.zeros((page_total,), jnp.float32).at[page_table.reshape(-1)].add(weights)
    owners = (new_slot // PAGE_DEV).astype(jnp.int32)
    summed = jax.ops.segment_sum(page_warmth, owners, num_segments=device_total)
    device_load = summed / (PPR * REQ_DEV)
    return migrated, device_load
```

```python
import functools

import jax
import jax.numpy as jnp
from jax import lax
from jax.experimental import pallas as pl
from jax.experimental.pallas import tpu as pltpu
from jax.sharding import PartitionSpec as P


AXES = ("node", "dev")
CHUNKS = 8
SMALL = 1 << 20
WIDE = 58 << 20
EARLY = 2


def quotient(value, size):
    if size & (size - 1) == 0:
        return lax.shift_right_logical(value, size.bit_length() - 1)
    return lax.div(value, size)


def remainder(value, size):
    if size & (size - 1) == 0:
        return lax.bitwise_and(value, size - 1)
    return lax.rem(value, size)


def exchange(x, mask):
    devices = lax.axis_size(AXES)
    return lax.ppermute(x, AXES, [(i, i ^ mask) for i in range(devices)])


def gather_order(devices):
    bits = devices.bit_length() - 1
    early = [1 << (bits - 1 - k) for k in range(EARLY)]
    late = [1 << k for k in range(bits - EARLY)]
    return early, late


def relative(position, masks):
    offset = 0
    for k, mask in enumerate(masks):
        offset = offset + ((position >> k) & 1) * mask
    return offset


def pack_kernel(me_ref, slot_ref, pages_ref, out_ref, page_of, held, in_sems, out_sems):
    devices, page_dev = out_ref.shape[0], pages_ref.shape[0]
    page_of[me_ref[0]] = 0

    def note(page, carry):
        page_of[quotient(slot_ref[page], page_dev)] = page
        return carry

    lax.fori_loop(0, page_dev, note, 0, unroll=16)

    def load(owner):
        return pltpu.make_async_copy(
            pages_ref.at[page_of[owner]], held.at[owner], in_sems.at[owner]
        )

    def store(owner):
        return pltpu.make_async_copy(
            held.at[owner], out_ref.at[owner], out_sems.at[owner]
        )

    def begin(owner, carry):
        load(owner).start()
        return carry

    def turn(owner, carry):
        load(owner).wait()
        store(owner).start()
        return carry

    def end(owner, carry):
        store(owner).wait()
        return carry

    lax.fori_loop(0, devices, begin, 0, unroll=8)
    lax.fori_loop(0, devices, turn, 0, unroll=8)
    lax.fori_loop(0, devices, end, 0, unroll=8)


def keep_kernel(pages_ref, out_ref, held, in_sems, out_sems):
    chunks, rows = held.shape[:2]
    loads = [
        pltpu.make_async_copy(
            pages_ref.at[pl.ds(c * rows, rows)], held.at[c], in_sems.at[c]
        )
        for c in range(chunks)
    ]
    stores = [
        pltpu.make_async_copy(
            held.at[c], out_ref.at[pl.ds(c * rows, rows)], out_sems.at[c]
        )
        for c in range(chunks)
    ]
    for load in loads:
        load.start()
    for load, store in zip(loads, stores):
        load.wait()
        store.start()
    for store in stores:
        store.wait()


def place_kernel(masks, me_ref, slot_ref, arrived_ref, kept_ref, out_ref, sems):
    del kept_ref
    devices = arrived_ref.shape[0]
    me = me_ref[0]
    copies = []
    for position in range(1, devices):
        source = me ^ relative(position, masks)
        copies.append(
            pltpu.make_async_copy(
                arrived_ref.at[source], out_ref.at[slot_ref[position]], sems.at[position]
            )
        )
    for copy in copies:
        copy.start()
    for copy in copies:
        copy.wait()


def heat_kernel(masks, devices, page_dev, me_ref, rate_ref, table_ref, out_ref):
    requests, listed = table_ref.shape
    high_of = relative(lax.broadcasted_iota(jnp.int32, (devices, listed), 0), masks) ^ me_ref[0]
    low_of = lax.broadcasted_iota(jnp.int32, (page_dev, listed), 0)
    total = jnp.zeros((devices, page_dev), jnp.float32)
    for r in range(requests):
        row = table_ref[r : r + 1, :]
        high = (quotient(row, page_dev) == high_of).astype(jnp.float32).astype(jnp.bfloat16)
        low = (remainder(row, page_dev) == low_of).astype(jnp.float32).astype(jnp.bfloat16)
        count = lax.dot_general(
            high, low, (((1,), (1,)), ((), ())), preferred_element_type=jnp.float32
        )
        total = total + rate_ref[r] * count
    out_ref[...] = total


def on_device(kv_pages, new_slot, request_rate, page_table):
    page_dev = kv_pages.shape[0]
    page_shape = kv_pages.shape[1:]
    devices = lax.axis_size(AXES)
    me = lax.axis_index(AXES).astype(jnp.int32)
    smem = pl.BlockSpec(memory_space=pltpu.SMEM)
    vmem = pl.BlockSpec(memory_space=pltpu.VMEM)
    anywhere = pl.BlockSpec(memory_space=pl.ANY)
    chunks = CHUNKS if page_dev % CHUNKS == 0 else 1
    early, late = gather_order(devices)
    masks = early + late

    slots = new_slot[None]
    for mask in early:
        slots = jnp.concatenate([slots, exchange(slots, mask)], axis=0)

    outgoing = pl.pallas_call(
        pack_kernel,
        out_shape=jax.ShapeDtypeStruct((devices,) + page_shape, kv_pages.dtype),
        in_specs=[smem, smem, anywhere],
        out_specs=anywhere,
        scratch_shapes=[
            pltpu.SMEM((devices,), jnp.int32),
            pltpu.VMEM((devices,) + page_shape, kv_pages.dtype),
            pltpu.SemaphoreType.DMA((devices,)),
            pltpu.SemaphoreType.DMA((devices,)),
        ],
        compiler_params=pltpu.CompilerParams(vmem_limit_bytes=WIDE),
        name="pack",
    )(me[None], new_slot, kv_pages)
    arrived = lax.all_to_all(outgoing, AXES, split_axis=0, concat_axis=0, tiled=True)

    heat = pl.pallas_call(
        functools.partial(heat_kernel, masks, devices, page_dev),
        out_shape=jax.ShapeDtypeStruct((devices, page_dev), jnp.float32),
        in_specs=[smem, smem, vmem],
        out_specs=vmem,
        compiler_params=pltpu.CompilerParams(vmem_limit_bytes=4 * SMALL),
        name="heat",
    )(me[None], request_rate, page_table)

    kept = pl.pallas_call(
        keep_kernel,
        out_shape=jax.ShapeDtypeStruct(kv_pages.shape, kv_pages.dtype),
        in_specs=[anywhere],
        out_specs=anywhere,
        scratch_shapes=[
            pltpu.VMEM((chunks, page_dev // chunks) + page_shape, kv_pages.dtype),
            pltpu.SemaphoreType.DMA((chunks,)),
            pltpu.SemaphoreType.DMA((chunks,)),
        ],
        compiler_params=pltpu.CompilerParams(
            vmem_limit_bytes=SMALL + kv_pages.size * kv_pages.dtype.itemsize
        ),
        name="keep",
        cost_estimate=pl.CostEstimate(
            flops=20_000_000_000, bytes_accessed=2 * kv_pages.size * 2, transcendentals=0
        ),
    )(kv_pages)

    for mask in late:
        slots = jnp.concatenate([slots, exchange(slots, mask)], axis=0)
    owners = quotient(slots, page_dev)
    arrived_slot = jnp.sum(jnp.where(owners == me, remainder(slots, page_dev), 0), axis=1)

    targets = jnp.arange(devices, dtype=jnp.int32)
    load = jnp.sum(
        jnp.where(owners[None] == targets[:, None, None], heat[None], 0.0), axis=(1, 2)
    )
    for mask in late:
        load = load + exchange(load, mask)
    offsets = [0]
    for mask in reversed(early):
        offsets = offsets + [o ^ mask for o in offsets]
    terms = [load if o == 0 else exchange(load, o) for o in offsets]
    while len(terms) > 1:
        terms = [a + b for a, b in zip(terms[::2], terms[1::2])]
    device_load = terms[0] / (page_table.shape[1] * page_table.shape[0])

    migrated = pl.pallas_call(
        functools.partial(place_kernel, masks),
        out_shape=jax.ShapeDtypeStruct(kv_pages.shape, kv_pages.dtype),
        in_specs=[smem, smem, anywhere, anywhere],
        out_specs=anywhere,
        scratch_shapes=[pltpu.SemaphoreType.DMA((devices,))],
        input_output_aliases={3: 0},
        compiler_params=pltpu.CompilerParams(vmem_limit_bytes=SMALL),
        name="place",
    )(me[None], arrived_slot, arrived, kept)
    return (migrated, device_load)


def solution(mesh):
    in_specs = (
        P(AXES, None, None, None, None),
        P(AXES),
        P(AXES),
        P(AXES, None),
    )
    out_specs = (P(AXES, None, None, None, None), P())

    return jax.shard_map(
        on_device, mesh=mesh, in_specs=in_specs, out_specs=out_specs, check_vma=False
    )
```

```python
import functools

import jax
import jax.numpy as jnp
from jax import lax
from jax.experimental import pallas as pl
from jax.experimental.pallas import tpu as pltpu
from jax.sharding import Mesh, PartitionSpec as P


AXIS = "all"
SMALL = 1 << 20
WIDE = 52 << 20
RELAYED = 2
PARTS = (8,)


def groups(devices):
    parity = lambda d: (d // (devices // 2) + d // 2) % 2
    return [[d for d in range(devices) if parity(d) == p] for p in (0, 1)]


def rank(device):
    return ((device >> 2) << 1) | (device & 1)


def quotient(value, size):
    if size & (size - 1) == 0:
        return lax.shift_right_logical(value, size.bit_length() - 1)
    return lax.div(value, size)


def remainder(value, size):
    if size & (size - 1) == 0:
        return lax.bitwise_and(value, size - 1)
    return lax.rem(value, size)


def exchange(x, mask):
    devices = lax.axis_size(AXIS)
    return lax.ppermute(x, AXIS, [(i, i ^ mask) for i in range(devices)])


def pair_masks(devices):
    half, eighth = devices // 2, devices // 8
    far = sorted((half + 4 * k for k in range(eighth)), key=lambda m: (-(m & 4), m))
    return far + [2 + 4 * k for k in range(eighth)]


def find_pages(slot_ref, page_of, page_dev, me):
    page_of[me] = 0

    def note(page, carry):
        page_of[quotient(slot_ref[page], page_dev)] = page
        return carry

    lax.fori_loop(0, page_dev, note, 0, unroll=16)


def pack_pairs_kernel(far, me_ref, slot_ref, pages_ref, *refs):
    pairs, swap_ref, page_of, sems = refs[:-3], *refs[-3:]
    me = me_ref[0]
    find_pages(slot_ref, page_of, pages_ref.shape[0], me)
    wanted = []
    for k, mask in enumerate(far):
        wanted.append((me ^ mask, pairs[k].at[0]))
        if k < RELAYED:
            wanted.append((me ^ mask ^ 1, pairs[k].at[1]))
        else:
            wanted.append((me ^ mask ^ 1, swap_ref.at[k - RELAYED]))
    copies = [
        pltpu.make_async_copy(pages_ref.at[page_of[owner]], target, sems.at[n])
        for n, (owner, target) in enumerate(wanted)
    ]
    for copy in copies:
        copy.start()
    for copy in copies:
        copy.wait()


def pack_group_kernel(me_ref, slot_ref, pages_ref, group_ref, page_of, held, in_sems, out_sems):
    count, page_dev = group_ref.shape[0], pages_ref.shape[0]
    me = me_ref[0]
    find_pages(slot_ref, page_of, page_dev, me)
    parity = quotient(me, count) ^ (quotient(me, 2) & 1)

    def member(r):
        return (r >> 1 << 2) + (parity ^ int(r >= count // 2)) * 2 + (r & 1)

    loads = [
        pltpu.make_async_copy(pages_ref.at[page_of[member(r)]], held.at[r], in_sems.at[r])
        for r in range(count)
    ]
    stores = [
        pltpu.make_async_copy(held.at[r], group_ref.at[r], out_sems.at[r])
        for r in range(count)
    ]
    for load in loads:
        load.start()
    for load, store in zip(loads, stores):
        load.wait()
        store.start()
    for store in stores:
        store.wait()


def join_kernel(swapped_ref, *refs):
    count = swapped_ref.shape[0]
    outs, sems = refs[count : 2 * count], refs[2 * count]
    copies = [
        pltpu.make_async_copy(swapped_ref.at[k], outs[k].at[1], sems.at[k])
        for k in range(count)
    ]
    for copy in copies:
        copy.start()
    for copy in copies:
        copy.wait()


def keep_kernel(first, rate_ref, table_ref, pages_ref, *refs):
    start, rows = first
    heat_ref = None
    if start:
        _, out_ref, held, in_sems, out_sems = refs
    else:
        out_ref, heat_ref, held, in_sems, out_sems = refs
    chunks = held.shape[0]
    part = lambda c: pl.ds((start + c) * rows, rows)
    loads = [
        pltpu.make_async_copy(pages_ref.at[part(c)], held.at[c], in_sems.at[c])
        for c in range(chunks)
    ]
    stores = [
        pltpu.make_async_copy(held.at[c], out_ref.at[part(c)], out_sems.at[c])
        for c in range(chunks)
    ]
    for load in loads:
        load.start()
    for load, store in zip(loads, stores):
        load.wait()
        store.start()
    if heat_ref is not None:
        heat_ref[...] = page_heat(rate_ref, table_ref, *heat_ref.shape)
    for store in stores:
        store.wait()


def page_heat(rate_ref, table_ref, devices, page_dev):
    requests, listed = table_ref.shape
    high_of = lax.broadcasted_iota(jnp.int32, (devices, listed), 0)
    low_of = lax.broadcasted_iota(jnp.int32, (page_dev, listed), 0)
    total = jnp.zeros((devices, page_dev), jnp.float32)
    for r in range(requests):
        row = table_ref[r : r + 1, :]
        high = (quotient(row, page_dev) == high_of).astype(jnp.float32).astype(jnp.bfloat16)
        low = (remainder(row, page_dev) == low_of).astype(jnp.float32).astype(jnp.bfloat16)
        count = lax.dot_general(
            high, low, (((1,), (1,)), ((), ())), preferred_element_type=jnp.float32
        )
        total = total + rate_ref[r] * count
    return total


def place_kernel(masks, slot_ref, me_ref, *refs):
    *arrived, relayed, group_ref, _, out_ref, sems = refs
    count = group_ref.shape[0]
    me = me_ref[0]
    copies = []

    def place(source, offset):
        slot = slot_ref[me ^ offset]
        copies.append(
            pltpu.make_async_copy(source, out_ref.at[slot], sems.at[len(copies)])
        )

    for k, mask in enumerate(masks):
        place(arrived[k].at[0], mask)
        place(relayed.at[k] if k < RELAYED else arrived[k].at[1], mask ^ 1)
    for offset in groups(2 * count)[0][1:]:
        place(group_ref.at[rank(me ^ offset)], offset)
    for copy in copies:
        copy.start()
    for copy in copies:
        copy.wait()


def on_device(kv_pages, new_slot, request_rate, page_table):
    page_dev = kv_pages.shape[0]
    page_shape = kv_pages.shape[1:]
    dtype = kv_pages.dtype
    devices = lax.axis_size(AXIS)
    me = lax.axis_index(AXIS).astype(jnp.int32)
    smem = pl.BlockSpec(memory_space=pltpu.SMEM)
    vmem = pl.BlockSpec(memory_space=pltpu.VMEM)
    anywhere = pl.BlockSpec(memory_space=pl.ANY)
    masks = pair_masks(devices)
    swaps = len(masks) - RELAYED
    pages = lambda count: jax.ShapeDtypeStruct((count,) + page_shape, dtype)
    wide = pltpu.CompilerParams(vmem_limit_bytes=WIDE)
    small = pltpu.CompilerParams(vmem_limit_bytes=SMALL)

    *pairs, swap = pl.pallas_call(
        functools.partial(pack_pairs_kernel, masks),
        out_shape=[pages(2) for _ in masks] + [pages(swaps)],
        in_specs=[smem, smem, anywhere],
        out_specs=[anywhere] * (len(masks) + 1),
        scratch_shapes=[
            pltpu.SMEM((devices,), jnp.int32),
            pltpu.SemaphoreType.DMA((devices,)),
        ],
        compiler_params=wide,
        name="pack_pairs",
    )(me[None], new_slot, kv_pages)
    swapped = exchange(swap, 1)
    joined = pl.pallas_call(
        join_kernel,
        out_shape=[pages(2)] * swaps,
        in_specs=[anywhere] * (swaps + 1),
        out_specs=[anywhere] * swaps,
        scratch_shapes=[pltpu.SemaphoreType.DMA((swaps,))],
        input_output_aliases={1 + k: k for k in range(swaps)},
        compiler_params=small,
        name="join",
    )(swapped, *pairs[RELAYED:])
    arrived = []
    for mask, pair in zip(masks, pairs[:RELAYED] + list(joined)):
        arrived.append(exchange(pair, mask))
    relayed = exchange(jnp.stack([a[1] for a in arrived[:RELAYED]]), 1)

    slots = lax.all_to_all(
        jnp.broadcast_to(new_slot[None], (devices, page_dev)),
        AXIS, split_axis=0, concat_axis=0, tiled=True,
    )
    owners = quotient(slots, page_dev)
    arrived_slot = jnp.sum(jnp.where(owners == me, remainder(slots, page_dev), 0), axis=1)

    group = pl.pallas_call(
        pack_group_kernel,
        out_shape=pages(devices // 2),
        in_specs=[smem, smem, anywhere],
        out_specs=anywhere,
        scratch_shapes=[
            pltpu.SMEM((devices,), jnp.int32),
            pltpu.VMEM((devices // 2,) + page_shape, dtype),
            pltpu.SemaphoreType.DMA((devices // 2,)),
            pltpu.SemaphoreType.DMA((devices // 2,)),
        ],
        compiler_params=wide,
        name="pack_group",
    )(me[None], new_slot, kv_pages)
    group = lax.all_to_all(
        group, AXIS, split_axis=0, concat_axis=0, tiled=True,
        axis_index_groups=groups(devices),
    )

    rows = page_dev // sum(PARTS)
    start, migrated, heat = 0, [], None
    for n, chunks in enumerate(PARTS):
        *migrated, = pl.pallas_call(
            functools.partial(keep_kernel, (start, rows)),
            out_shape=[jax.ShapeDtypeStruct(kv_pages.shape, dtype)]
            + [jax.ShapeDtypeStruct((devices, page_dev), jnp.float32)] * (n == 0),
            in_specs=[smem, vmem, anywhere] + [anywhere] * (n > 0),
            out_specs=[anywhere] + [vmem] * (n == 0),
            scratch_shapes=[
                pltpu.VMEM((chunks, rows) + page_shape, dtype),
                pltpu.SemaphoreType.DMA((chunks,)),
                pltpu.SemaphoreType.DMA((chunks,)),
            ],
            input_output_aliases={3: 0} if n else {},
            compiler_params=wide,
            cost_estimate=pl.CostEstimate(
                flops=5_000_000_000, bytes_accessed=kv_pages.size, transcendentals=0
            ),
        )(request_rate, page_table, kv_pages, *migrated[:1])
        if n == 0:
            heat = migrated[1]
        start += chunks

    targets = jnp.arange(devices, dtype=jnp.int32)
    load = jnp.sum(
        jnp.where(owners[None] == targets[:, None, None], heat[None], 0.0), axis=(1, 2)
    )
    early, late = sum_masks(devices)
    for mask in late:
        load = load + exchange(load, mask)
    terms = [load]
    for offset in (early[1], early[0], early[0] ^ early[1]):
        terms.append(exchange(load, offset))
    load = (terms[0] + terms[1]) + (terms[2] + terms[3])
    device_load = load / (page_table.shape[1] * page_table.shape[0])

    migrated = pl.pallas_call(
        functools.partial(place_kernel, masks),
        out_shape=jax.ShapeDtypeStruct(kv_pages.shape, dtype),
        in_specs=[smem, smem] + [anywhere] * (len(masks) + 3),
        out_specs=anywhere,
        scratch_shapes=[pltpu.SemaphoreType.DMA((devices,))],
        input_output_aliases={len(masks) + 4: 0},
        compiler_params=small,
        name="place",
    )(arrived_slot, me[None], *arrived, relayed, group, migrated[0])
    return (migrated, device_load)


def sum_masks(devices):
    bits = devices.bit_length() - 1
    return [1 << (bits - 1), 1 << (bits - 2)], [1 << k for k in range(bits - 2)]


def solution(mesh):
    devices = mesh.devices.size
    flat = Mesh(mesh.devices.reshape(devices), (AXIS,))
    in_specs = (
        P(AXIS, None, None, None, None),
        P(AXIS),
        P(AXIS),
        P(AXIS, None),
    )
    out_specs = (P(AXIS, None, None, None, None), P())

    return jax.shard_map(
        on_device, mesh=flat, in_specs=in_specs, out_specs=out_specs, check_vma=False
    )
```

```python
import functools

import jax
import jax.numpy as jnp
from jax import lax
from jax.experimental import pallas as pl
from jax.experimental.pallas import tpu as pltpu
from jax.sharding import Mesh, PartitionSpec as P


AXIS = "all"
SMALL = 1 << 20
WIDE = 52 << 20
RELAYED = 3
PARTS = (8,)


def groups(devices):
    parity = lambda d: (d // (devices // 2) + d // 2) % 2
    return [[d for d in range(devices) if parity(d) == p] for p in (0, 1)]


def rank(device):
    return ((device >> 2) << 1) | (device & 1)


def quotient(value, size):
    if size & (size - 1) == 0:
        return lax.shift_right_logical(value, size.bit_length() - 1)
    return lax.div(value, size)


def remainder(value, size):
    if size & (size - 1) == 0:
        return lax.bitwise_and(value, size - 1)
    return lax.rem(value, size)


def exchange(x, mask):
    devices = lax.axis_size(AXIS)
    return lax.ppermute(x, AXIS, [(i, i ^ mask) for i in range(devices)])


def pair_masks(devices):
    half, eighth = devices // 2, devices // 8
    far = sorted((half + 4 * k for k in range(eighth)), key=lambda m: (-(m & 4), m))
    return far + [2 + 4 * k for k in range(eighth)]


def find_pages(slot_ref, page_of, page_dev, me):
    page_of[me] = 0

    def note(page, carry):
        page_of[quotient(slot_ref[page], page_dev)] = page
        return carry

    lax.fori_loop(0, page_dev, note, 0, unroll=16)


def pack_pairs_kernel(far, me_ref, slot_ref, row_ref, pages_ref, *refs):
    pairs, (swap_ref, rows_ref, page_of, sems, row_sems) = refs[:-5], refs[-5:]
    me = me_ref[0]
    rows = [
        pltpu.make_async_copy(row_ref, rows_ref.at[d, 0], row_sems.at[d])
        for d in range(rows_ref.shape[0])
    ]
    find_pages(slot_ref, page_of, pages_ref.shape[0], me)
    wanted = []
    for k, mask in enumerate(far):
        wanted.append((me ^ mask, pairs[k].at[0]))
        if k < RELAYED:
            wanted.append((me ^ mask ^ 1, pairs[k].at[1]))
        else:
            wanted.append((me ^ mask ^ 1, swap_ref.at[k - RELAYED]))
    copies = [
        pltpu.make_async_copy(pages_ref.at[page_of[owner]], target, sems.at[n])
        for n, (owner, target) in enumerate(wanted)
    ]
    for copy in copies + rows:
        copy.start()
    for copy in copies + rows:
        copy.wait()


def pack_group_kernel(me_ref, slot_ref, pages_ref, group_ref, page_of, held, in_sems, out_sems):
    count, page_dev = group_ref.shape[0], pages_ref.shape[0]
    me = me_ref[0]
    find_pages(slot_ref, page_of, page_dev, me)
    parity = quotient(me, count) ^ (quotient(me, 2) & 1)

    def member(r):
        return (r >> 1 << 2) + (parity ^ int(r >= count // 2)) * 2 + (r & 1)

    loads = [
        pltpu.make_async_copy(pages_ref.at[page_of[member(r)]], held.at[r], in_sems.at[r])
        for r in range(count)
    ]
    stores = [
        pltpu.make_async_copy(held.at[r], group_ref.at[r], out_sems.at[r])
        for r in range(count)
    ]
    for load in loads:
        load.start()
    for load, store in zip(loads, stores):
        load.wait()
        store.start()
    for store in stores:
        store.wait()


def join_kernel(swapped_ref, *refs):
    count = swapped_ref.shape[0]
    outs, sems = refs[count : 2 * count], refs[2 * count]
    copies = [
        pltpu.make_async_copy(swapped_ref.at[k], outs[k].at[1], sems.at[k])
        for k in range(count)
    ]
    for copy in copies:
        copy.start()
    for copy in copies:
        copy.wait()


def keep_kernel(first, rate_ref, table_ref, pages_ref, *refs):
    start, rows = first
    heat_ref = None
    if start:
        _, out_ref, held, in_sems, out_sems = refs
    else:
        out_ref, heat_ref, held, in_sems, out_sems = refs
    chunks = held.shape[0]
    part = lambda c: pl.ds((start + c) * rows, rows)
    loads = [
        pltpu.make_async_copy(pages_ref.at[part(c)], held.at[c], in_sems.at[c])
        for c in range(chunks)
    ]
    stores = [
        pltpu.make_async_copy(held.at[c], out_ref.at[part(c)], out_sems.at[c])
        for c in range(chunks)
    ]
    for load in loads:
        load.start()
    for load, store in zip(loads, stores):
        load.wait()
        store.start()
    if heat_ref is not None:
        heat_ref[...] = page_heat(rate_ref, table_ref, *heat_ref.shape)
    for store in stores:
        store.wait()


def page_heat(rate_ref, table_ref, devices, page_dev):
    requests, listed = table_ref.shape
    high_of = lax.broadcasted_iota(jnp.int32, (devices, listed), 0)
    low_of = lax.broadcasted_iota(jnp.int32, (page_dev, listed), 0)
    total = jnp.zeros((devices, page_dev), jnp.float32)
    for r in range(requests):
        row = table_ref[r : r + 1, :]
        high = (quotient(row, page_dev) == high_of).astype(jnp.float32).astype(jnp.bfloat16)
        low = (remainder(row, page_dev) == low_of).astype(jnp.float32).astype(jnp.bfloat16)
        count = lax.dot_general(
            high, low, (((1,), (1,)), ((), ())), preferred_element_type=jnp.float32
        )
        total = total + rate_ref[r] * count
    return total


def place_kernel(masks, slot_ref, me_ref, *refs):
    *arrived, relayed, group_ref, _, out_ref, sems = refs
    count = group_ref.shape[0]
    me = me_ref[0]
    copies = []

    def place(source, offset):
        slot = slot_ref[me ^ offset]
        copies.append(
            pltpu.make_async_copy(source, out_ref.at[slot], sems.at[len(copies)])
        )

    for k, mask in enumerate(masks):
        place(arrived[k].at[0], mask)
        place(relayed.at[k] if k < RELAYED else arrived[k].at[1], mask ^ 1)
    for offset in groups(2 * count)[0][1:]:
        place(group_ref.at[rank(me ^ offset)], offset)
    for copy in copies:
        copy.start()
    for copy in copies:
        copy.wait()


def on_device(kv_pages, new_slot, request_rate, page_table):
    page_dev = kv_pages.shape[0]
    page_shape = kv_pages.shape[1:]
    dtype = kv_pages.dtype
    devices = lax.axis_size(AXIS)
    me = lax.axis_index(AXIS).astype(jnp.int32)
    smem = pl.BlockSpec(memory_space=pltpu.SMEM)
    vmem = pl.BlockSpec(memory_space=pltpu.VMEM)
    anywhere = pl.BlockSpec(memory_space=pl.ANY)
    masks = pair_masks(devices)
    swaps = len(masks) - RELAYED
    pages = lambda count: jax.ShapeDtypeStruct((count,) + page_shape, dtype)
    wide = pltpu.CompilerParams(vmem_limit_bytes=WIDE)
    small = pltpu.CompilerParams(vmem_limit_bytes=SMALL)

    *pairs, swap, rows = pl.pallas_call(
        functools.partial(pack_pairs_kernel, masks),
        out_shape=[pages(2) for _ in masks]
        + [pages(swaps), jax.ShapeDtypeStruct((devices, 1, page_dev), jnp.int32)],
        in_specs=[smem, smem, anywhere, anywhere],
        out_specs=[anywhere] * (len(masks) + 2),
        scratch_shapes=[
            pltpu.SMEM((devices,), jnp.int32),
            pltpu.SemaphoreType.DMA((devices,)),
            pltpu.SemaphoreType.DMA((devices,)),
        ],
        compiler_params=wide,
        name="pack_pairs",
    )(me[None], new_slot, new_slot, kv_pages)
    swapped = exchange(swap, 1)
    joined = pl.pallas_call(
        join_kernel,
        out_shape=[pages(2)] * swaps,
        in_specs=[anywhere] * (swaps + 1),
        out_specs=[anywhere] * swaps,
        scratch_shapes=[pltpu.SemaphoreType.DMA((swaps,))],
        input_output_aliases={1 + k: k for k in range(swaps)},
        compiler_params=small,
        name="join",
    )(swapped, *pairs[RELAYED:])
    arrived = []
    for mask, pair in zip(masks, pairs[:RELAYED] + list(joined)):
        arrived.append(exchange(pair, mask))
    relayed = exchange(jnp.stack([a[1] for a in arrived[:RELAYED]]), 1)

    slots = lax.all_to_all(rows, AXIS, split_axis=0, concat_axis=0, tiled=True)
    slots = slots.reshape(devices, page_dev)
    owners = quotient(slots, page_dev)
    arrived_slot = jnp.sum(jnp.where(owners == me, remainder(slots, page_dev), 0), axis=1)

    group = pl.pallas_call(
        pack_group_kernel,
        out_shape=pages(devices // 2),
        in_specs=[smem, smem, anywhere],
        out_specs=anywhere,
        scratch_shapes=[
            pltpu.SMEM((devices,), jnp.int32),
            pltpu.VMEM((devices // 2,) + page_shape, dtype),
            pltpu.SemaphoreType.DMA((devices // 2,)),
            pltpu.SemaphoreType.DMA((devices // 2,)),
        ],
        compiler_params=wide,
        name="pack_group",
    )(me[None], new_slot, kv_pages)
    group = lax.all_to_all(
        group, AXIS, split_axis=0, concat_axis=0, tiled=True,
        axis_index_groups=groups(devices),
    )

    height = page_dev // sum(PARTS)
    start, migrated, heat = 0, [], None
    for n, chunks in enumerate(PARTS):
        *migrated, = pl.pallas_call(
            functools.partial(keep_kernel, (start, height)),
            out_shape=[jax.ShapeDtypeStruct(kv_pages.shape, dtype)]
            + [jax.ShapeDtypeStruct((devices, page_dev), jnp.float32)] * (n == 0),
            in_specs=[smem, vmem, anywhere] + [anywhere] * (n > 0),
            out_specs=[anywhere] + [vmem] * (n == 0),
            scratch_shapes=[
                pltpu.VMEM((chunks, height) + page_shape, dtype),
                pltpu.SemaphoreType.DMA((chunks,)),
                pltpu.SemaphoreType.DMA((chunks,)),
            ],
            input_output_aliases={3: 0} if n else {},
            compiler_params=wide,
            cost_estimate=pl.CostEstimate(
                flops=5_000_000_000, bytes_accessed=kv_pages.size, transcendentals=0
            ),
        )(request_rate, page_table, kv_pages, *migrated[:1])
        if n == 0:
            heat = migrated[1]
        start += chunks

    targets = jnp.arange(devices, dtype=jnp.int32)
    load = jnp.sum(
        jnp.where(owners[None] == targets[:, None, None], heat[None], 0.0), axis=(1, 2)
    )
    early, late = sum_masks(devices)
    for mask in late:
        load = load + exchange(load, mask)
    terms = [load]
    for offset in (early[1], early[0], early[0] ^ early[1]):
        terms.append(exchange(load, offset))
    load = (terms[0] + terms[1]) + (terms[2] + terms[3])
    device_load = load / (page_table.shape[1] * page_table.shape[0])

    migrated = pl.pallas_call(
        functools.partial(place_kernel, masks),
        out_shape=jax.ShapeDtypeStruct(kv_pages.shape, dtype),
        in_specs=[smem, smem] + [anywhere] * (len(masks) + 3),
        out_specs=anywhere,
        scratch_shapes=[pltpu.SemaphoreType.DMA((devices,))],
        input_output_aliases={len(masks) + 4: 0},
        compiler_params=small,
        name="place",
    )(arrived_slot, me[None], *arrived, relayed, group, migrated[0])
    return (migrated, device_load)


def sum_masks(devices):
    bits = devices.bit_length() - 1
    return [1 << (bits - 1), 1 << (bits - 2)], [1 << k for k in range(bits - 2)]


def solution(mesh):
    devices = mesh.devices.size
    flat = Mesh(mesh.devices.reshape(devices), (AXIS,))
    in_specs = (
        P(AXIS, None, None, None, None),
        P(AXIS),
        P(AXIS),
        P(AXIS, None),
    )
    out_specs = (P(AXIS, None, None, None, None), P())

    return jax.shard_map(
        on_device, mesh=flat, in_specs=in_specs, out_specs=out_specs, check_vma=False
    )
```
